32 devices in a mesh: row: 4 (over x, core), col: 8 (over z, y).
Axes of the slice: x: 2, y: 2, z: 4, core: 2. Of those that a mesh axis runs over, the one named last changes fastest.
Arguments:
- tokens: bfloat16 [2048, 4096], P('col', 'row'), may hold values from -6 to 6
- gate_weight: bfloat16 [4096, 2048], P('row', 'col'), may hold values from -0.125 to 0.125
- up_weight: bfloat16 [4096, 2048], P('row', 'col'), may hold values from -0.125 to 0.125
- down_weight: bfloat16 [2048, 4096], P('col', 'row'), may hold values from -0.1875 to 0.1875
- gate_mask: int32 [16, 8], P('row', 'col'), may hold values from 0 to 1, as said below
- up_mask: int32 [16, 8], P('row', 'col'), may hold values from 0 to 1, as said below
- down_mask: int32 [8, 16], P('col', 'row'), may hold values from 0 to 1, as said below
Outputs:
- layer_out: bfloat16 [2048, 4096], P('col', 'row')
The draws below stay inside these ranges and needn't reach their ends.
Inputs may be any that keep to these rules, and one draw needn't show every extreme that they name: `gate_mask`: every entry is 0 or 1; tile rows differ strongly in how many ones they hold, some rows nearly empty and some nearly full. `up_mask`: every entry is 0 or 1; tile rows differ strongly in how many ones they hold, some rows nearly empty and some nearly full. `down_mask`: every entry is 0 or 1; tile rows differ strongly in how many ones they hold, some rows nearly empty and some nearly full.
All inputs are finite; a program needn't handle non-finite values.
Results may differ from the reference program's by a relative error of at most 0.025.
Values may be sent and summed in bfloat16 or wider, within the bound.
A program may use at most 64 MiB of HBM per device.

```python
import jax
import jax.numpy as jnp
from jax import lax

D = 4096
TILE = 256
TOKENS = 2048
FF = 2048
ROW_FEATURES = 1024
N_ROW = 4


def skewed_tiles(key, tile_rows, tile_cols):
    row_level = jax.random.randint(jax.random.fold_in(key, 1), (tile_rows, 1), 0, 4)
    tile_coin = jax.random.randint(jax.random.fold_in(key, 2), (tile_rows, tile_cols), 0, 8)
    return (tile_coin < 1 + 2 * row_level).astype(jnp.int32)


def draw_gate_mask(key, part):
    return skewed_tiles(jax.random.fold_in(key, 11), D // TILE, FF // TILE)


def draw_up_mask(key, part):
    return skewed_tiles(jax.random.fold_in(key, 12), D // TILE, FF // TILE)


def draw_down_mask(key, part):
    return skewed_tiles(jax.random.fold_in(key, 13), FF // TILE, D // TILE)


def shard_levels(rng, dims, pieces, low, high):
    factor_of, own = 1.0, jax.random.fold_in(rng, 6)
    for position, parts in pieces:
        draws = jnp.exp(jax.random.uniform(jax.random.fold_in(own, position), (parts,), jnp.float32, low / len(pieces), high / len(pieces)))
        factor_of = factor_of * jnp.repeat(draws, dims[position] // parts).reshape([-1 if axis == position else 1 for axis in range(len(dims))])
    return factor_of


def noise(key, extent, spread, bound, shards=(), dtype=jnp.bfloat16):
    array = spread * jax.random.normal(key, extent, jnp.float32)
    if shards:
        array = array * shard_levels(key, extent, shards, -0.22, 0.18)
    return jnp.clip(array, -bound, bound).astype(dtype)


def setup_inputs(seed: int = 0) -> dict:
    key_list = jax.random.split(jax.random.key(seed), 8)
    return {
        "tokens": noise(key_list[0], (TOKENS, D), 1.0, 6.0, ((0, 8), (1, 4))),
        "gate_weight": noise(key_list[1], (D, FF), (D // 2) ** -0.5, 0.125, ((0, 4), (1, 8))),
        "up_weight": noise(key_list[2], (D, FF), (D // 2) ** -0.5, 0.125, ((0, 4), (1, 8))),
        "down_weight": noise(key_list[3], (FF, D), (FF // 2) ** -0.5, 0.1875, ((0, 8), (1, 4))),
        "gate_mask": draw_gate_mask(jax.random.fold_in(key_list[7], 71), 0),
        "up_mask": draw_up_mask(jax.random.fold_in(key_list[7], 71), 0),
        "down_mask": draw_down_mask(jax.random.fold_in(key_list[7], 71), 0),
    }


def widen_mask(tile_mask):
    return jnp.repeat(jnp.repeat(tile_mask, TILE, axis=0), TILE, axis=1).astype(jnp.bfloat16)


def row_blocks(tokens, weight):
    summed = jnp.zeros((TOKENS, FF), jnp.float32)
    for group in range(N_ROW):
        lower = group * ROW_FEATURES
        partial_value = jnp.dot(tokens[:, lower:lower + ROW_FEATURES], weight[lower:lower + ROW_FEATURES, :], preferred_element_type=jnp.float32)
        rounded = lax.optimization_barrier(partial_value.astype(jnp.bfloat16))
        summed = summed + rounded.astype(jnp.float32)
    return summed


def reference(tokens, gate_weight, up_weight, down_weight, gate_mask, up_mask, down_mask):
    masked_gate = gate_weight * widen_mask(gate_mask)
    masked_up = up_weight * widen_mask(up_mask)
    masked_down = down_weight * widen_mask(down_mask)
    gate_sum = row_blocks(tokens, masked_gate)
    up_sum = row_blocks(tokens, masked_up)
    hidden = (jax.nn.silu(gate_sum) * up_sum).astype(jnp.bfloat16)
    return jnp.dot(hidden, masked_down, preferred_element_type=jnp.float32).astype(jnp.bfloat16)
```

```python
import functools

import jax
import jax.numpy as jnp
from jax import lax
from jax.experimental import pallas as pl
from jax.experimental.pallas import tpu as pltpu
from jax.sharding import PartitionSpec as P

MESH = pl.DeviceIdType.MESH
F32 = jnp.float32
BF16 = jnp.bfloat16
PAIR = 2
PIECES = 2


def pick(table, index):
    out = jnp.int32(table[0])
    for place, value in enumerate(table):
        if place:
            out = jnp.where(index == place, jnp.int32(value), out)
    return out


def arrival_orders(line):
    orders = []
    for a in range(line):
        orders.append(sorted(range(line), key=lambda b: (abs(b - a), b)))
    return orders


def reduce_orders(line):
    orders = []
    for a in range(line):
        orders.append(sorted((b for b in range(line) if b != a), key=lambda b: (-abs(b - a), b)))
    return orders


def kernel(
    line, xs,
    tok_hbm, gate_hbm, up_hbm, down_hbm, gmask, umask, dmask, out_hbm,
    xbuf, raw, rawd, w, wd, zsend, zrecv, zown, xsend, xrecv, hbuf, psend, pleft, pright, pown, obuf,
    loc, ag_r, ag_l, ag_in, wsem, cz_s, cz_r, xz_s, xz_r, xh_s, xh_r, ch_s, ch_r, p_s, pl_r, pr_r,
):
    row = lax.axis_index("row")
    col = lax.axis_index("col")
    core, x = row % 2, row // 2
    y, a = col % PAIR, col // PAIR
    tokens, k = tok_hbm.shape
    units = gate_hbm.shape[1]
    half = tokens // 2
    part = half // xs
    peer_core = {"row": x * 2 + 1 - core, "col": col}
    peer_y = {"row": row, "col": a * PAIR + 1 - y}
    right = {"row": row, "col": (a + 1) * PAIR + y}
    left = {"row": row, "col": (a - 1) * PAIR + y}
    has_right, has_left = a < line - 1, a > 0

    def at_x(d):
        return {"row": lax.rem(x + d, xs) * 2 + core, "col": col}

    def remote(src, dst, s, r, dev):
        return pltpu.make_async_remote_copy(
            src_ref=src, dst_ref=dst, send_sem=s, recv_sem=r, device_id=dev, device_id_type=MESH
        )

    loads = [
        pltpu.make_async_copy(tok_hbm, xbuf.at[a], loc.at[0]),
        pltpu.make_async_copy(gate_hbm, raw.at[0], loc.at[1]),
        pltpu.make_async_copy(up_hbm, raw.at[1], loc.at[2]),
        pltpu.make_async_copy(down_hbm, rawd, loc.at[3]),
    ]
    for c in loads:
        c.start()

    barrier = pltpu.get_barrier_semaphore()

    def greet(dev):
        pl.semaphore_signal(barrier, inc=1, device_id=dev, device_id_type=MESH)

    greet(peer_core)
    greet(peer_y)
    for d in range(1, xs):
        greet(at_x(d))

    @pl.when(has_right)
    def _():
        greet(right)

    @pl.when(has_left)
    def _():
        greet(left)

    ends = has_right.astype(jnp.int32) + has_left.astype(jnp.int32)
    pl.semaphore_wait(barrier, 1 + xs + ends)

    def go_right(b):
        return remote(xbuf.at[b], xbuf.at[b], ag_r.at[b], ag_in.at[b], right)

    def go_left(b):
        return remote(xbuf.at[b], xbuf.at[b], ag_l.at[b], ag_in.at[b], left)

    loads[0].wait()

    @pl.when(has_right)
    def _():
        go_right(a).start()

    @pl.when(has_left)
    def _():
        go_left(a).start()

    tile = k // gmask.shape[0]
    for which, mask in ((0, gmask), (1, umask)):
        loads[1 + which].wait()
        for i in range(mask.shape[0]):
            keep = mask[i, 0].astype(F32)
            rows = pl.ds(i * tile, tile)
            w[0, which, rows, :] = (raw[which, rows, :].astype(F32) * keep).astype(BF16)
    w_copy = remote(w.at[0], w.at[1], wsem.at[0], wsem.at[1], peer_y)
    w_copy.start()
    loads[3].wait()
    wide = down_hbm.shape[1] // dmask.shape[1]
    for i in range(dmask.shape[1]):
        keep = dmask[0, i].astype(F32)
        cols = pl.ds(i * wide, wide)
        wd[0, :, cols] = (rawd[:, cols].astype(F32) * keep).astype(BF16)
    d_copy = remote(wd.at[0], wd.at[1], wsem.at[2], wsem.at[3], peer_y)
    d_copy.start()

    arrive = arrival_orders(line)
    order = [pick([arrive[i][j] for i in range(line)], a) for j in range(line)]

    def take(j):
        b = order[j]
        go_right(b).wait_recv()

        @pl.when((b < a) & has_right)
        def _():
            go_right(b).start()

        @pl.when((b > a) & has_left)
        def _():
            go_left(b).start()

    def core_copy(s):
        return remote(zsend.at[s], zrecv.at[s], cz_s.at[s], cz_r.at[s], peer_core)

    def project(j, h):
        s = j * 2 + h
        b = order[j]

        def dots(rows):
            lhs = xbuf[b, rows, :]
            return [jnp.dot(lhs, w[h, i], preferred_element_type=F32) for i in range(2)]

        other = dots(pl.ds(pl.multiple_of((1 - core) * half, half), half))
        for i in range(2):
            zsend[s, i] = other[i].astype(BF16)
        core_copy(s).start()
        mine = dots(pl.ds(pl.multiple_of(core * half, half), half))
        for i in range(2):
            zown[s, i] = mine[i]

    def x_copy(s, d):
        to = lax.rem(x + d, xs)
        return remote(xsend.at[s, to], xrecv.at[s, d], xz_s.at[s, d], xz_r.at[s, d], at_x(d))

    def fold_core(s):
        core_copy(s).wait_recv()
        for i in range(2):
            total = zown[s, i] + zrecv[s, i].astype(F32)
            zown[s, i] = total
            for to in range(xs):
                xsend[s, to, i] = total[to * part:(to + 1) * part].astype(BF16)
        for d in range(1, xs):
            x_copy(s, d).start()

    def h_copy(s, d):
        return remote(hbuf.at[s, core, x], hbuf.at[s, core, x], xh_s.at[s, d], xh_r.at[s, d], at_x(d))

    def activate(s):
        rows = pl.ds(pl.multiple_of(x * part, part), part)
        acc = [zown[s, i, rows, :] for i in range(2)]
        for d in range(1, xs):
            x_copy(s, d).wait_recv()
            for i in range(2):
                acc[i] = acc[i] + xrecv[s, d, i].astype(F32)
        g, u = acc
        hbuf[s, core, x] = (g / (1.0 + jnp.exp(-g)) * u).astype(BF16)
        for d in range(1, xs):
            h_copy(s, d).start()

    def hc_copy(s):
        return remote(hbuf.at[s, core], hbuf.at[s, core], ch_s.at[s], ch_r.at[s], peer_core)

    def share(s):
        for d in range(1, xs):
            h_copy(s, d).wait_recv()
        hc_copy(s).start()

    def settle(s):
        hc_copy(s).wait_recv()

    def rest(group):
        for stage in (fold_core, activate, share, settle):
            for j, h in group:
                stage(j * 2 + h)

    middle = has_left & has_right
    first = [(j, 0) for j in range(line - 1)]
    second = [(j, 1) for j in range(line - 1)]
    third = [(line - 1, 0), (line - 1, 1)]
    for j, h in first:
        if j:
            take(j)
        project(j, h)
    rest(first)
    w_copy.wait_recv()
    for j, h in second:
        project(j, h)

    @pl.when(middle)
    def _():
        take(line - 1)

    rest(second)

    @pl.when(jnp.logical_not(middle))
    def _():
        take(line - 1)

    for j, h in third:
        project(j, h)
    rest(third)
    d_copy.wait_recv()

    size = tokens // PIECES
    far = reduce_orders(line)
    home = list(range(line))

    def term(j, q):
        acc = None
        for h in range(2):
            hid = hbuf[j * 2 + h].reshape(tokens, units)[q * size:(q + 1) * size]
            t = jnp.dot(hid, wd[h], preferred_element_type=F32)
            acc = t if acc is None else acc + t
        return acc

    def p_right(b, q):
        return remote(psend.at[b, q], pleft.at[b, q], p_s.at[b, q], pl_r.at[b, q], right)

    def p_left(b, q):
        return remote(psend.at[b, q], pright.at[b, q], p_s.at[b, q], pr_r.at[b, q], left)

    for j in range(line - 1, 0, -1):
        b = order[j]
        for q in range(PIECES):
            pown[...] = term(j, q)

            @pl.when((b > a) & has_left)
            def _():
                p_right(b, q).wait_recv()
                pown[...] += pleft[b, q].astype(F32)

            @pl.when((b < a) & has_right)
            def _():
                p_left(b, q).wait_recv()
                pown[...] += pright[b, q].astype(F32)

            psend[b, q] = pown[...].astype(BF16)

            @pl.when(b > a)
            def _():
                p_right(b, q).start()

            @pl.when(b < a)
            def _():
                p_left(b, q).start()

    for q in range(PIECES):
        pown[...] = term(0, q)

        @pl.when(has_left)
        def _():
            p_right(a, q).wait_recv()
            pown[...] += pleft[a, q].astype(F32)

        @pl.when(has_right)
        def _():
            p_left(a, q).wait_recv()
            pown[...] += pright[a, q].astype(F32)

        obuf[pl.ds(q * size, size), :] = pown[...].astype(BF16)
        pltpu.make_async_copy(
            obuf.at[pl.ds(q * size, size), :], out_hbm.at[pl.ds(q * size, size), :], loc.at[4 + q]
        ).start()

    w_copy.wait_send()
    d_copy.wait_send()
    for j in range(line):
        b = order[j]

        @pl.when((b <= a) & has_right)
        def _():
            go_right(b).wait_send()

        @pl.when((b >= a) & has_left)
        def _():
            go_left(b).wait_send()

        if j:
            for q in range(PIECES):
                p_right(b, q).wait_send()
        for h in range(2):
            s = j * 2 + h
            core_copy(s).wait_send()
            hc_copy(s).wait_send()
            for d in range(1, xs):
                x_copy(s, d).wait_send()
                h_copy(s, d).wait_send()
    for q in range(PIECES):
        pltpu.make_async_copy(
            obuf.at[pl.ds(q * size, size), :], out_hbm.at[pl.ds(q * size, size), :], loc.at[4 + q]
        ).wait()


def per_device(n_row, n_col, tokens, gate, up, down, gmask, umask, dmask):
    line, xs = n_col // PAIR, n_row // 2
    t, k = tokens.shape
    units = gate.shape[1]
    wide = down.shape[1]
    half = t // 2
    part = half // xs
    steps = 2 * line
    dma = pltpu.SemaphoreType.DMA
    vmem = pltpu.VMEM
    hbm = pl.BlockSpec(memory_space=pl.ANY)
    smem = pl.BlockSpec(memory_space=pltpu.SMEM)
    size = t // PIECES
    return pl.pallas_call(
        functools.partial(kernel, line, xs),
        out_shape=jax.ShapeDtypeStruct((t, wide), BF16),
        in_specs=[hbm] * 4 + [smem] * 3,
        out_specs=hbm,
        scratch_shapes=[
            vmem((line, t, k), BF16),
            vmem((2, k, units), BF16),
            vmem((units, wide), BF16),
            vmem((2, 2, k, units), BF16),
            vmem((2, units, wide), BF16),
            vmem((steps, 2, half, units), BF16),
            vmem((steps, 2, half, units), BF16),
            vmem((steps, 2, half, units), F32),
            vmem((steps, xs, 2, part, units), BF16),
            vmem((steps, xs, 2, part, units), BF16),
            vmem((steps, 2, xs, part, units), BF16),
            vmem((line, PIECES, size, wide), BF16),
            vmem((line, PIECES, size, wide), BF16),
            vmem((line, PIECES, size, wide), BF16),
            vmem((size, wide), F32),
            vmem((t, wide), BF16),
            dma((4 + PIECES,)),
            dma((line,)), dma((line,)), dma((line,)),
            dma((4,)),
            dma((steps,)), dma((steps,)),
            dma((steps, xs)), dma((steps, xs)),
            dma((steps, xs)), dma((steps, xs)),
            dma((steps,)), dma((steps,)),
            dma((line, PIECES)), dma((line, PIECES)), dma((line, PIECES)),
        ],
        compiler_params=pltpu.CompilerParams(
            collective_id=0, has_side_effects=True, vmem_limit_bytes=60 * 1024 * 1024
        ),
    )(tokens, gate, up, down, gmask, umask, dmask)


def solution(mesh):
    n_row, n_col = mesh.shape["row"], mesh.shape["col"]
    return jax.shard_map(
        functools.partial(per_device, n_row, n_col),
        mesh=mesh,
        in_specs=(
            P("col", "row"),
            P("row", "col"),
            P("row", "col"),
            P("col", "row"),
            P("row", "col"),
            P("row", "col"),
            P("col", "row"),
        ),
        out_specs=P("col", "row"),
        check_vma=False,
    )
```

```python
import functools

import jax
import jax.numpy as jnp
from jax import lax
from jax.experimental import pallas as pl
from jax.experimental.pallas import tpu as pltpu
from jax.sharding import PartitionSpec as P

MESH = pl.DeviceIdType.MESH
F32 = jnp.float32
BF16 = jnp.bfloat16
PAIR = 2
PIECES = 4
HALVES = 2


def pick(table, index):
    out = jnp.int32(table[0])
    for place, value in enumerate(table):
        if place:
            out = jnp.where(index == place, jnp.int32(value), out)
    return out


def arrival_orders(line):
    return [sorted(range(line), key=lambda b: (abs(b - a), b)) for a in range(line)]


def reduce_orders(line):
    sends = [line - 2, line - 1] + list(range(line - 3, 0, -1))
    rank = {b: 2 * place for place, b in enumerate(sends)}

    def key(a, b):
        return rank[b] + a if b > a else rank[line - 1 - b] + line - 1 - a

    return [
        sorted((b for b in range(line) if b != a), key=lambda b: (key(a, b), b)) for a in range(line)
    ]


def kernel(
    line, xs, tiles, down_tiles,
    tok_hbm, gate_hbm, up_hbm, down_hbm, gmask, umask, dmask, out_hbm,
    xbuf, raw, rawd, w, wd, zsend, zrecv, zown, xsend, xrecv, hbuf, psend, pleft, pright, pown, obuf,
    loc, ag_r, ag_l, ag_in, wsem, cz_s, cz_r, xz_s, xz_r, xh_s, xh_r, ch_s, ch_r, p_s, pl_r, pr_r,
):
    row = lax.axis_index("row")
    col = lax.axis_index("col")
    core, x = row % 2, row // 2
    y, a = col % PAIR, col // PAIR
    _, half, k = tok_hbm.shape
    tokens = 2 * half
    units = gate_hbm.shape[1]
    part = half // xs
    peer_core = {"row": x * 2 + 1 - core, "col": col}
    peer_y = {"row": row, "col": a * PAIR + 1 - y}
    right = {"row": row, "col": (a + 1) * PAIR + y}
    left = {"row": row, "col": (a - 1) * PAIR + y}
    has_right, has_left = a < line - 1, a > 0

    def at_x(d):
        return {"row": lax.rem(x + d, xs) * 2 + core, "col": col}

    def remote(src, dst, s, r, dev):
        return pltpu.make_async_remote_copy(
            src_ref=src, dst_ref=dst, send_sem=s, recv_sem=r, device_id=dev, device_id_type=MESH
        )

    loads = [
        pltpu.make_async_copy(tok_hbm, xbuf.at[a], loc.at[0]),
        pltpu.make_async_copy(gate_hbm, raw.at[0], loc.at[1]),
        pltpu.make_async_copy(up_hbm, raw.at[1], loc.at[2]),
        pltpu.make_async_copy(down_hbm, rawd, loc.at[3]),
    ]
    for c in loads:
        c.start()

    barrier = pltpu.get_barrier_semaphore()

    def greet(dev):
        pl.semaphore_signal(barrier, inc=1, device_id=dev, device_id_type=MESH)

    greet(peer_core)
    greet(peer_y)
    for d in range(1, xs):
        greet(at_x(d))

    @pl.when(has_right)
    def _():
        greet(right)

    @pl.when(has_left)
    def _():
        greet(left)

    ends = has_right.astype(jnp.int32) + has_left.astype(jnp.int32)
    pl.semaphore_wait(barrier, 1 + xs + ends)

    def go_right(b, q):
        return remote(xbuf.at[b, q], xbuf.at[b, q], ag_r.at[b, q], ag_in.at[b, q], right)

    def go_left(b, q):
        return remote(xbuf.at[b, q], xbuf.at[b, q], ag_l.at[b, q], ag_in.at[b, q], left)

    loads[0].wait()
    for q in range(HALVES):

        @pl.when(has_right)
        def _():
            go_right(a, q).start()

        @pl.when(has_left)
        def _():
            go_left(a, q).start()

    for which, mask in ((0, gmask), (1, umask)):
        loads[1 + which].wait()
        n_row, n_col = tiles
        for i in range(n_row):
            for j in range(n_col):
                keep = mask[i * n_col + j].astype(F32)
                rows = pl.ds(i * (k // n_row), k // n_row)
                cols = pl.ds(j * (units // n_col), units // n_col)
                w[0, which, rows, cols] = (raw[which, rows, cols].astype(F32) * keep).astype(BF16)
    w_copy = remote(w.at[0], w.at[1], wsem.at[0], wsem.at[1], peer_y)
    w_copy.start()
    loads[3].wait()
    n_row, n_col = down_tiles
    wide = down_hbm.shape[1]
    for i in range(n_row):
        for j in range(n_col):
            keep = dmask[i * n_col + j].astype(F32)
            rows = pl.ds(i * (units // n_row), units // n_row)
            cols = pl.ds(j * (wide // n_col), wide // n_col)
            wd[0, rows, cols] = (rawd[rows, cols].astype(F32) * keep).astype(BF16)
    d_copy = remote(wd.at[0], wd.at[1], wsem.at[2], wsem.at[3], peer_y)
    d_copy.start()

    arrive = arrival_orders(line)
    order = [pick([arrive[i][j] for i in range(line)], a) for j in range(line)]

    def take(j, q):
        b = order[j]
        go_right(b, q).wait_recv()

        @pl.when((b < a) & has_right)
        def _():
            go_right(b, q).start()

        @pl.when((b > a) & has_left)
        def _():
            go_left(b, q).start()

    def core_copy(s):
        return remote(zsend.at[s], zrecv.at[s], cz_s.at[s], cz_r.at[s], peer_core)

    def project(j, h):
        s = j * 2 + h
        b = order[j]

        def dots(which):
            lhs = xbuf[b, which]
            return [jnp.dot(lhs, w[h, i], preferred_element_type=F32) for i in range(2)]

        other = dots(1 - core)
        for i in range(2):
            zsend[s, i] = other[i].astype(BF16)
        core_copy(s).start()
        mine = dots(core)
        for i in range(2):
            zown[s, i] = mine[i]

    def x_copy(s, d):
        to = lax.rem(x + d, xs)
        return remote(xsend.at[s, to], xrecv.at[s, d], xz_s.at[s, d], xz_r.at[s, d], at_x(d))

    def fold_core(s):
        core_copy(s).wait_recv()
        for i in range(2):
            total = zown[s, i] + zrecv[s, i].astype(F32)
            zown[s, i] = total
            for to in range(xs):
                xsend[s, to, i] = total[to * part:(to + 1) * part].astype(BF16)
        for d in range(1, xs):
            x_copy(s, d).start()

    def h_copy(s, d):
        return remote(hbuf.at[s, core, x], hbuf.at[s, core, x], xh_s.at[s, d], xh_r.at[s, d], at_x(d))

    def activate(s):
        rows = pl.ds(pl.multiple_of(x * part, part), part)
        acc = [zown[s, i, rows, :] for i in range(2)]
        for d in range(1, xs):
            x_copy(s, d).wait_recv()
            for i in range(2):
                acc[i] = acc[i] + xrecv[s, d, i].astype(F32)
        g, u = acc
        hbuf[s, core, x] = (g / (1.0 + jnp.exp(-g)) * u).astype(BF16)
        for d in range(1, xs):
            h_copy(s, d).start()

    def hc_copy(s):
        return remote(hbuf.at[s, core], hbuf.at[s, core], ch_s.at[s], ch_r.at[s], peer_core)

    def share(s):
        for d in range(1, xs):
            h_copy(s, d).wait_recv()
        hc_copy(s).start()

    def settle(s):
        hc_copy(s).wait_recv()

    def rest(group):
        for stage in (fold_core, activate, share, settle):
            for j, h in group:
                stage(j * 2 + h)

    middle = has_left & has_right
    outer = jnp.logical_not(middle)
    last = line - 1
    second = [(j, 1) for j in range(last)]
    third = [(last, 0), (last, 1)]

    project(0, 0)
    rest([(0, 0)])

    @pl.when(middle)
    def _():
        for low in range(1, last, 2):
            for q in range(HALVES):
                for j in range(low, min(low + 2, last)):
                    take(j, q)

    for j in range(1, last):

        @pl.when(outer)
        def _():
            for q in range(HALVES):
                take(j, q)

        project(j, 0)
    rest([(j, 0) for j in range(1, last)])

    @pl.when(middle)
    def _():
        for q in range(HALVES):
            take(last, q)

    w_copy.wait_recv()
    for j, h in second:
        project(j, h)

    @pl.when(middle)
    def _():
        for j, h in third:
            project(j, h)
        rest(second + third)

    @pl.when(outer)
    def _():
        rest(second)

    d_copy.wait_recv()

    size = tokens // PIECES
    far = reduce_orders(line)
    targets = [pick([far[i][n] for i in range(line)], a) for n in range(last)]
    spots = [pick([arrive[i].index(far[i][n]) for i in range(line)], a) for n in range(last)]

    def term(j, q):
        acc = None
        for h in range(2):
            hid = hbuf[j * 2 + h].reshape(tokens, units)[q * size:(q + 1) * size]
            t = jnp.dot(hid, wd[h], preferred_element_type=F32)
            acc = t if acc is None else acc + t
        return acc

    def p_right(b, q):
        return remote(psend.at[b, q], pleft.at[b, q], p_s.at[b, q], pl_r.at[b, q], right)

    def p_left(b, q):
        return remote(psend.at[b, q], pright.at[b, q], p_s.at[b, q], pr_r.at[b, q], left)

    def reduce(n):
        b = targets[n]
        for q in range(PIECES):
            pown[...] = term(spots[n], q)

            @pl.when((b > a) & has_left)
            def _():
                p_right(b, q).wait_recv()
                pown[...] += pleft[b, q].astype(F32)

            @pl.when((b < a) & has_right)
            def _():
                p_left(b, q).wait_recv()
                pown[...] += pright[b, q].astype(F32)

            psend[b, q] = pown[...].astype(BF16)

            @pl.when(b > a)
            def _():
                p_right(b, q).start()

            @pl.when(b < a)
            def _():
                p_left(b, q).start()

    reduce(0)

    @pl.when(outer)
    def _():
        for q in range(HALVES):
            take(last, q)
        for j, h in third:
            project(j, h)
        rest(third)

    for n in range(1, last):
        reduce(n)

    for q in range(PIECES):
        pown[...] = term(0, q)

        @pl.when(has_left)
        def _():
            p_right(a, q).wait_recv()
            pown[...] += pleft[a, q].astype(F32)

        @pl.when(has_right)
        def _():
            p_left(a, q).wait_recv()
            pown[...] += pright[a, q].astype(F32)

        obuf[pl.ds(q * size, size), :] = pown[...].astype(BF16)
        pltpu.make_async_copy(
            obuf.at[pl.ds(q * size, size), :], out_hbm.at[pl.ds(q * size, size), :], loc.at[4 + q]
        ).start()

    w_copy.wait_send()
    d_copy.wait_send()
    for j in range(line):
        b = order[j]

        for q in range(HALVES):

            @pl.when((b <= a) & has_right)
            def _():
                go_right(b, q).wait_send()

            @pl.when((b >= a) & has_left)
            def _():
                go_left(b, q).wait_send()

        if j:
            for q in range(PIECES):
                p_right(b, q).wait_send()
        for h in range(2):
            s = j * 2 + h
            core_copy(s).wait_send()
            hc_copy(s).wait_send()
            for d in range(1, xs):
                x_copy(s, d).wait_send()
                h_copy(s, d).wait_send()
    for q in range(PIECES):
        pltpu.make_async_copy(
            obuf.at[pl.ds(q * size, size), :], out_hbm.at[pl.ds(q * size, size), :], loc.at[4 + q]
        ).wait()


def per_device(n_row, n_col, tokens, gate, up, down, gmask, umask, dmask):
    line, xs = n_col // PAIR, n_row // 2
    t, k = tokens.shape
    units = gate.shape[1]
    wide = down.shape[1]
    half = t // 2
    part = half // xs
    steps = 2 * line
    dma = pltpu.SemaphoreType.DMA
    vmem = pltpu.VMEM
    hbm = pl.BlockSpec(memory_space=pl.ANY)
    smem = pl.BlockSpec(memory_space=pltpu.SMEM)
    size = t // PIECES
    return pl.pallas_call(
        functools.partial(kernel, line, xs, gmask.shape, dmask.shape),
        out_shape=jax.ShapeDtypeStruct((t, wide), BF16),
        in_specs=[hbm] * 4 + [smem] * 3,
        out_specs=hbm,
        scratch_shapes=[
            vmem((line, HALVES, half, k), BF16),
            vmem((2, k, units), BF16),
            vmem((units, wide), BF16),
            vmem((2, 2, k, units), BF16),
            vmem((2, units, wide), BF16),
            vmem((steps, 2, half, units), BF16),
            vmem((steps, 2, half, units), BF16),
            vmem((steps, 2, half, units), F32),
            vmem((steps, xs, 2, part, units), BF16),
            vmem((steps, xs, 2, part, units), BF16),
            vmem((steps, 2, xs, part, units), BF16),
            vmem((line, PIECES, size, wide), BF16),
            vmem((line, PIECES, size, wide), BF16),
            vmem((line, PIECES, size, wide), BF16),
            vmem((size, wide), F32),
            vmem((t, wide), BF16),
            dma((4 + PIECES,)),
            dma((line, HALVES)), dma((line, HALVES)), dma((line, HALVES)),
            dma((4,)),
            dma((steps,)), dma((steps,)),
            dma((steps, xs)), dma((steps, xs)),
            dma((steps, xs)), dma((steps, xs)),
            dma((steps,)), dma((steps,)),
            dma((line, PIECES)), dma((line, PIECES)), dma((line, PIECES)),
        ],
        compiler_params=pltpu.CompilerParams(
            collective_id=0, has_side_effects=True, vmem_limit_bytes=60 * 1024 * 1024
        ),
    )(tokens.reshape(HALVES, half, k), gate, up, down, *(m.reshape(-1) for m in (gmask, umask, dmask)))


def solution(mesh):
    n_row, n_col = mesh.shape["row"], mesh.shape["col"]
    return jax.shard_map(
        functools.partial(per_device, n_row, n_col),
        mesh=mesh,
        in_specs=(
            P("col", "row"),
            P("row", "col"),
            P("row", "col"),
            P("col", "row"),
            P("row", "col"),
            P("row", "col"),
            P("col", "row"),
        ),
        out_specs=P("col", "row"),
        check_vma=False,
    )
```

```python
import functools

import jax
import jax.numpy as jnp
from jax import lax
from jax.experimental import pallas as pl
from jax.experimental.pallas import tpu as pltpu
from jax.sharding import PartitionSpec as P

MESH = pl.DeviceIdType.MESH
F32 = jnp.float32
BF16 = jnp.bfloat16
PAIR = 2
PIECES = 4
HALVES = 2


def pick(table, index):
    out = jnp.int32(table[0])
    for place, value in enumerate(table):
        if place:
            out = jnp.where(index == place, jnp.int32(value), out)
    return out


def arrival_orders(line):
    return [sorted(range(line), key=lambda b: (abs(b - a), b)) for a in range(line)]


def reduce_orders(line):
    sends = [line - 2, line - 1] + list(range(line - 3, 0, -1))
    rank = {b: 2 * place for place, b in enumerate(sends)}

    def key(a, b):
        return rank[b] + a if b > a else rank[line - 1 - b] + line - 1 - a

    return [
        sorted((b for b in range(line) if b != a), key=lambda b: (key(a, b), b)) for a in range(line)
    ]


def kernel(
    line, xs, tiles, down_tiles,
    tok_hbm, gate_hbm, up_hbm, down_hbm, gmask, umask, dmask, out_hbm,
    xbuf, raw, rawd, w, wd, zsend, zrecv, zown, xsend, xrecv, hbuf, psend, pleft, pright, pown, obuf,
    loc, ag_r, ag_l, ag_in, wsem, d_s, d_r, cz_s, cz_r, xz_s, xz_r, xh_s, xh_r, ch_s, ch_r, p_s, pl_r, pr_r,
):
    row = lax.axis_index("row")
    col = lax.axis_index("col")
    core, x = row % 2, row // 2
    y, a = col % PAIR, col // PAIR
    _, half, k = tok_hbm.shape
    tokens = 2 * half
    units = gate_hbm.shape[1]
    part = half // xs
    peer_core = {"row": x * 2 + 1 - core, "col": col}
    peer_y = {"row": row, "col": a * PAIR + 1 - y}
    right = {"row": row, "col": (a + 1) * PAIR + y}
    left = {"row": row, "col": (a - 1) * PAIR + y}
    has_right, has_left = a < line - 1, a > 0

    def at_x(d):
        return {"row": lax.rem(x + d, xs) * 2 + core, "col": col}

    def remote(src, dst, s, r, dev):
        return pltpu.make_async_remote_copy(
            src_ref=src, dst_ref=dst, send_sem=s, recv_sem=r, device_id=dev, device_id_type=MESH
        )

    loads = [
        pltpu.make_async_copy(tok_hbm, xbuf.at[a], loc.at[0]),
        pltpu.make_async_copy(gate_hbm, raw.at[0], loc.at[1]),
        pltpu.make_async_copy(up_hbm, raw.at[1], loc.at[2]),
        pltpu.make_async_copy(down_hbm, rawd, loc.at[3]),
    ]
    for c in loads:
        c.start()

    barrier = pltpu.get_barrier_semaphore()

    def greet(dev):
        pl.semaphore_signal(barrier, inc=1, device_id=dev, device_id_type=MESH)

    greet(peer_core)
    greet(peer_y)
    for d in range(1, xs):
        greet(at_x(d))

    @pl.when(has_right)
    def _():
        greet(right)

    @pl.when(has_left)
    def _():
        greet(left)

    ends = has_right.astype(jnp.int32) + has_left.astype(jnp.int32)
    pl.semaphore_wait(barrier, 1 + xs + ends)

    def go_right(b, q):
        return remote(xbuf.at[b, q], xbuf.at[b, q], ag_r.at[b, q], ag_in.at[b, q], right)

    def go_left(b, q):
        return remote(xbuf.at[b, q], xbuf.at[b, q], ag_l.at[b, q], ag_in.at[b, q], left)

    loads[0].wait()
    for q in range(HALVES):

        @pl.when(has_right)
        def _():
            go_right(a, q).start()

        @pl.when(has_left)
        def _():
            go_left(a, q).start()

    for which, mask in ((0, gmask), (1, umask)):
        loads[1 + which].wait()
        n_row, n_col = tiles
        for i in range(n_row):
            for j in range(n_col):
                keep = mask[i * n_col + j].astype(F32)
                rows = pl.ds(i * (k // n_row), k // n_row)
                cols = pl.ds(j * (units // n_col), units // n_col)
                w[0, which, rows, cols] = (raw[which, rows, cols].astype(F32) * keep).astype(BF16)
    w_copy = remote(w.at[0], w.at[1], wsem.at[0], wsem.at[1], peer_y)
    w_copy.start()
    loads[3].wait()
    n_row, n_col = down_tiles
    wide = down_hbm.shape[1]
    for i in range(n_row):
        for j in range(n_col):
            keep = dmask[i * n_col + j].astype(F32)
            rows = pl.ds(i * (units // n_row), units // n_row)
            cols = pl.ds(j * (wide // n_col), wide // n_col)
            rawd[rows, cols] = (rawd[rows, cols].astype(F32) * keep).astype(BF16)
    size = wide // PIECES
    for q in range(PIECES):
        wd[0, q] = rawd[:, q * size:(q + 1) * size]
    def d_copy(q):
        return remote(wd.at[0, q], wd.at[1, q], d_s.at[q], d_r.at[q], peer_y)

    for q in range(PIECES):
        d_copy(q).start()

    arrive = arrival_orders(line)
    order = [pick([arrive[i][j] for i in range(line)], a) for j in range(line)]

    def take(j, q):
        b = order[j]
        go_right(b, q).wait_recv()

        @pl.when((b < a) & has_right)
        def _():
            go_right(b, q).start()

        @pl.when((b > a) & has_left)
        def _():
            go_left(b, q).start()

    def core_copy(s):
        return remote(zsend.at[s], zrecv.at[s], cz_s.at[s], cz_r.at[s], peer_core)

    def project(j, h):
        s = j * 2 + h
        b = order[j]

        for i in range(2):
            both = jnp.dot(
                xbuf[b].reshape(tokens, k), w[h, i], preferred_element_type=F32
            )
            for q in range(HALVES):
                zown[s, q, i] = both[q * half:(q + 1) * half]
            zsend[s, i] = zown[s, 1 - core, i].astype(BF16)
        core_copy(s).start()

    def x_copy(s, d):
        to = lax.rem(x + d, xs)
        return remote(xsend.at[s, to], xrecv.at[s, d], xz_s.at[s, d], xz_r.at[s, d], at_x(d))

    def fold_core(s):
        core_copy(s).wait_recv()
        for i in range(2):
            total = zown[s, core, i] + zrecv[s, i].astype(F32)
            zown[s, core, i] = total
            for to in range(xs):
                xsend[s, to, i] = total[to * part:(to + 1) * part].astype(BF16)
        for d in range(1, xs):
            x_copy(s, d).start()

    def h_copy(s, d):
        return remote(hbuf.at[s, core, x], hbuf.at[s, core, x], xh_s.at[s, d], xh_r.at[s, d], at_x(d))

    def activate(s):
        rows = pl.ds(pl.multiple_of(x * part, part), part)
        acc = [zown[s, core, i, rows, :] for i in range(2)]
        for d in range(1, xs):
            x_copy(s, d).wait_recv()
            for i in range(2):
                acc[i] = acc[i] + xrecv[s, d, i].astype(F32)
        g, u = acc
        hbuf[s, core, x] = (g / (1.0 + jnp.exp(-g)) * u).astype(BF16)
        for d in range(1, xs):
            h_copy(s, d).start()

    def hc_copy(s):
        return remote(hbuf.at[s, core], hbuf.at[s, core], ch_s.at[s], ch_r.at[s], peer_core)

    def share(s):
        for d in range(1, xs):
            h_copy(s, d).wait_recv()
        hc_copy(s).start()

    def settle(s):
        hc_copy(s).wait_recv()

    def rest(group):
        for stage in (fold_core, activate, share, settle):
            for j, h in group:
                stage(j * 2 + h)

    middle = has_left & has_right
    outer = jnp.logical_not(middle)
    last = line - 1
    second = [(j, 1) for j in range(last - 1, -1, -1)]
    third = [(last, 0), (last, 1)]

    project(0, 0)
    rest([(0, 0)])

    @pl.when(middle)
    def _():
        for low in range(1, last, 2):
            for q in range(HALVES):
                for j in range(low, min(low + 2, last)):
                    take(j, q)

    for j in range(1, last):

        @pl.when(outer)
        def _():
            for q in range(HALVES):
                take(j, q)

        project(j, 0)
    rest([(j, 0) for j in range(1, last)])

    @pl.when(middle)
    def _():
        for q in range(HALVES):
            take(last, q)

    far = reduce_orders(line)
    targets = [pick([far[i][n] for i in range(line)], a) for n in range(last)]
    spots = [pick([arrive[i].index(far[i][n]) for i in range(line)], a) for n in range(last)]

    def term(j, q):
        acc = None
        for h in range(2):
            hid = hbuf[j * 2 + h].reshape(tokens, units)
            t = jnp.dot(hid, wd[h, q], preferred_element_type=F32)
            acc = t if acc is None else acc + t
        return acc

    def p_right(b, q):
        return remote(psend.at[b, q], pleft.at[b, q], p_s.at[b, q], pl_r.at[b, q], right)

    def p_left(b, q):
        return remote(psend.at[b, q], pright.at[b, q], p_s.at[b, q], pr_r.at[b, q], left)

    def reduce(n):
        b = targets[n]
        for q in range(PIECES):
            if n == 0:
                d_copy(q).wait_recv()
            pown[...] = term(spots[n], q)

            @pl.when((b > a) & has_left)
            def _():
                p_right(b, q).wait_recv()
                pown[...] += pleft[b, q].astype(F32)

            @pl.when((b < a) & has_right)
            def _():
                p_left(b, q).wait_recv()
                pown[...] += pright[b, q].astype(F32)

            psend[b, q] = pown[...].astype(BF16)

            @pl.when(b > a)
            def _():
                p_right(b, q).start()

            @pl.when(b < a)
            def _():
                p_left(b, q).start()

    w_copy.wait_recv()
    for j, h in second:
        project(j, h)

    @pl.when(middle)
    def _():
        for j, h in third:
            project(j, h)
        rest(second + third)
        reduce(0)

    @pl.when(outer)
    def _():
        rest(second)
        for q in range(HALVES):
            take(last, q)
        for j, h in third:
            project(j, h)
        reduce(0)
        rest(third)

    for n in range(1, last):
        reduce(n)

    for q in range(PIECES):
        pown[...] = term(0, q)

        @pl.when(has_left)
        def _():
            p_right(a, q).wait_recv()
            pown[...] += pleft[a, q].astype(F32)

        @pl.when(has_right)
        def _():
            p_left(a, q).wait_recv()
            pown[...] += pright[a, q].astype(F32)

        obuf[:, pl.ds(q * size, size)] = pown[...].astype(BF16)
        pltpu.make_async_copy(
            obuf.at[:, pl.ds(q * size, size)], out_hbm.at[:, pl.ds(q * size, size)], loc.at[4 + q]
        ).start()

    w_copy.wait_send()
    for q in range(PIECES):
        d_copy(q).wait_send()
    for j in range(line):
        b = order[j]

        for q in range(HALVES):

            @pl.when((b <= a) & has_right)
            def _():
                go_right(b, q).wait_send()

            @pl.when((b >= a) & has_left)
            def _():
                go_left(b, q).wait_send()

        if j:
            for q in range(PIECES):
                p_right(b, q).wait_send()
        for h in range(2):
            s = j * 2 + h
            core_copy(s).wait_send()
            hc_copy(s).wait_send()
            for d in range(1, xs):
                x_copy(s, d).wait_send()
                h_copy(s, d).wait_send()
    for q in range(PIECES):
        pltpu.make_async_copy(
            obuf.at[:, pl.ds(q * size, size)], out_hbm.at[:, pl.ds(q * size, size)], loc.at[4 + q]
        ).wait()


def per_device(n_row, n_col, tokens, gate, up, down, gmask, umask, dmask):
    line, xs = n_col // PAIR, n_row // 2
    t, k = tokens.shape
    units = gate.shape[1]
    wide = down.shape[1]
    half = t // 2
    part = half // xs
    steps = 2 * line
    dma = pltpu.SemaphoreType.DMA
    vmem = pltpu.VMEM
    hbm = pl.BlockSpec(memory_space=pl.ANY)
    smem = pl.BlockSpec(memory_space=pltpu.SMEM)
    size = wide // PIECES
    return pl.pallas_call(
        functools.partial(kernel, line, xs, gmask.shape, dmask.shape),
        out_shape=jax.ShapeDtypeStruct((t, wide), BF16),
        in_specs=[hbm] * 4 + [smem] * 3,
        out_specs=hbm,
        scratch_shapes=[
            vmem((line, HALVES, half, k), BF16),
            vmem((2, k, units), BF16),
            vmem((units, wide), BF16),
            vmem((2, 2, k, units), BF16),
            vmem((2, PIECES, units, size), BF16),
            vmem((steps, 2, half, units), BF16),
            vmem((steps, 2, half, units), BF16),
            vmem((steps, HALVES, 2, half, units), F32),
            vmem((steps, xs, 2, part, units), BF16),
            vmem((steps, xs, 2, part, units), BF16),
            vmem((steps, 2, xs, part, units), BF16),
            vmem((line, PIECES, t, size), BF16),
            vmem((line, PIECES, t, size), BF16),
            vmem((line, PIECES, t, size), BF16),
            vmem((t, size), F32),
            vmem((t, wide), BF16),
            dma((4 + PIECES,)),
            dma((line, HALVES)), dma((line, HALVES)), dma((line, HALVES)),
            dma((2,)), dma((PIECES,)), dma((PIECES,)),
            dma((steps,)), dma((steps,)),
            dma((steps, xs)), dma((steps, xs)),
            dma((steps, xs)), dma((steps, xs)),
            dma((steps,)), dma((steps,)),
            dma((line, PIECES)), dma((line, PIECES)), dma((line, PIECES)),
        ],
        compiler_params=pltpu.CompilerParams(
            collective_id=0, has_side_effects=True, vmem_limit_bytes=60 * 1024 * 1024
        ),
    )(tokens.reshape(HALVES, half, k), gate, up, down, *(m.reshape(-1) for m in (gmask, umask, dmask)))


def solution(mesh):
    n_row, n_col = mesh.shape["row"], mesh.shape["col"]
    return jax.shard_map(
        functools.partial(per_device, n_row, n_col),
        mesh=mesh,
        in_specs=(
            P("col", "row"),
            P("row", "col"),
            P("row", "col"),
            P("col", "row"),
            P("row", "col"),
            P("row", "col"),
            P("col", "row"),
        ),
        out_specs=P("col", "row"),
        check_vma=False,
    )
```

```python
import functools

import jax
import jax.numpy as jnp
from jax import lax
from jax.experimental import pallas as pl
from jax.experimental.pallas import tpu as pltpu
from jax.sharding import PartitionSpec as P

MESH = pl.DeviceIdType.MESH
F32 = jnp.float32
BF16 = jnp.bfloat16
PAIR = 2
PIECES = 4
HALVES = 2


def pick(table, index):
    out = jnp.int32(table[0])
    for place, value in enumerate(table):
        if place:
            out = jnp.where(index == place, jnp.int32(value), out)
    return out


def arrival_orders(line):
    return [sorted(range(line), key=lambda b: (abs(b - a), b)) for a in range(line)]


def reduce_orders(line):
    sends = [line - 2, line - 1] + list(range(line - 3, 0, -1))
    rank = {b: 2 * place for place, b in enumerate(sends)}

    def key(a, b):
        return rank[b] + a if b > a else rank[line - 1 - b] + line - 1 - a

    return [
        sorted((b for b in range(line) if b != a), key=lambda b: (key(a, b), b)) for a in range(line)
    ]


def kernel(
    line, xs, tiles, down_tiles,
    tok_hbm, gate_hbm, up_hbm, down_hbm, gmask, umask, dmask, out_hbm,
    xbuf, raw, rawd, w, wd, zsend, zrecv, zown, xsend, xrecv, hbuf, psend, pleft, pright, pown, obuf,
    loc, ag_r, ag_l, ag_in, wsem, d_s, d_r, cz_s, cz_r, xz_s, xz_r, xh_s, xh_r, ch_s, ch_r, p_s, pl_r, pr_r,
):
    row = lax.axis_index("row")
    col = lax.axis_index("col")
    core, x = row % 2, row // 2
    y, a = col % PAIR, col // PAIR
    _, half, k = tok_hbm.shape
    tokens = 2 * half
    units = gate_hbm.shape[1]
    part = half // xs
    peer_core = {"row": x * 2 + 1 - core, "col": col}
    peer_y = {"row": row, "col": a * PAIR + 1 - y}
    right = {"row": row, "col": (a + 1) * PAIR + y}
    left = {"row": row, "col": (a - 1) * PAIR + y}
    has_right, has_left = a < line - 1, a > 0

    def at_x(d):
        return {"row": lax.rem(x + d, xs) * 2 + core, "col": col}

    def remote(src, dst, s, r, dev):
        return pltpu.make_async_remote_copy(
            src_ref=src, dst_ref=dst, send_sem=s, recv_sem=r, device_id=dev, device_id_type=MESH
        )

    loads = [
        pltpu.make_async_copy(tok_hbm, xbuf.at[a], loc.at[0]),
        pltpu.make_async_copy(gate_hbm, raw.at[0], loc.at[1]),
        pltpu.make_async_copy(up_hbm, raw.at[1], loc.at[2]),
        pltpu.make_async_copy(down_hbm, rawd, loc.at[3]),
    ]
    for c in loads:
        c.start()

    barrier = pltpu.get_barrier_semaphore()

    def greet(dev):
        pl.semaphore_signal(barrier, inc=1, device_id=dev, device_id_type=MESH)

    greet(peer_core)
    greet(peer_y)
    for d in range(1, xs):
        greet(at_x(d))

    @pl.when(has_right)
    def _():
        greet(right)

    @pl.when(has_left)
    def _():
        greet(left)

    ends = has_right.astype(jnp.int32) + has_left.astype(jnp.int32)
    pl.semaphore_wait(barrier, 1 + xs + ends)

    def go_right(b, q):
        return remote(xbuf.at[b, q], xbuf.at[b, q], ag_r.at[b, q], ag_in.at[b, q], right)

    def go_left(b, q):
        return remote(xbuf.at[b, q], xbuf.at[b, q], ag_l.at[b, q], ag_in.at[b, q], left)

    loads[0].wait()
    for q in range(HALVES):

        @pl.when(has_right)
        def _():
            go_right(a, q).start()

        @pl.when(has_left)
        def _():
            go_left(a, q).start()

    for which, mask in ((0, gmask), (1, umask)):
        loads[1 + which].wait()
        n_row, n_col = tiles
        for i in range(n_row):
            for j in range(n_col):
                keep = mask[i * n_col + j].astype(F32)
                rows = pl.ds(i * (k // n_row), k // n_row)
                cols = pl.ds(j * (units // n_col), units // n_col)
                w[0, which, rows, cols] = (raw[which, rows, cols].astype(F32) * keep).astype(BF16)
    w_copy = remote(w.at[0], w.at[1], wsem.at[0], wsem.at[1], peer_y)
    w_copy.start()
    loads[3].wait()
    n_row, n_col = down_tiles
    wide = down_hbm.shape[1]
    for i in range(n_row):
        for j in range(n_col):
            keep = dmask[i * n_col + j].astype(F32)
            rows = pl.ds(i * (units // n_row), units // n_row)
            cols = pl.ds(j * (wide // n_col), wide // n_col)
            rawd[rows, cols] = (rawd[rows, cols].astype(F32) * keep).astype(BF16)
    size = wide // PIECES
    for q in range(PIECES):
        wd[0, q] = rawd[:, q * size:(q + 1) * size]
    def d_copy(q):
        return remote(wd.at[0, q], wd.at[1, q], d_s.at[q], d_r.at[q], peer_y)

    for q in range(PIECES):
        d_copy(q).start()

    arrive = arrival_orders(line)
    order = [pick([arrive[i][j] for i in range(line)], a) for j in range(line)]

    def take(j, q):
        b = order[j]
        go_right(b, q).wait_recv()

        @pl.when((b < a) & has_right)
        def _():
            go_right(b, q).start()

        @pl.when((b > a) & has_left)
        def _():
            go_left(b, q).start()

    def core_copy(s):
        return remote(zsend.at[s], zrecv.at[s], cz_s.at[s], cz_r.at[s], peer_core)

    def project(j, h):
        s = j * 2 + h
        b = order[j]

        for i in range(2):
            both = jnp.dot(
                xbuf[b].reshape(tokens, k), w[h, i], preferred_element_type=F32
            )
            for q in range(HALVES):
                zown[s, q, i] = both[q * half:(q + 1) * half]
            zsend[s, i] = zown[s, 1 - core, i].astype(BF16)
        core_copy(s).start()

    def x_copy(s, d):
        to = lax.rem(x + d, xs)
        return remote(xsend.at[s, to], xrecv.at[s, d], xz_s.at[s, d], xz_r.at[s, d], at_x(d))

    def fold_core(s):
        core_copy(s).wait_recv()
        for i in range(2):
            total = zown[s, core, i] + zrecv[s, i].astype(F32)
            zown[s, core, i] = total
            for to in range(xs):
                xsend[s, to, i] = total[to * part:(to + 1) * part].astype(BF16)
        for d in range(1, xs):
            x_copy(s, d).start()

    def h_copy(s, d):
        return remote(hbuf.at[s, core, x], hbuf.at[s, core, x], xh_s.at[s, d], xh_r.at[s, d], at_x(d))

    def activate(s):
        rows = pl.ds(pl.multiple_of(x * part, part), part)
        acc = [zown[s, core, i, rows, :] for i in range(2)]
        for d in range(1, xs):
            x_copy(s, d).wait_recv()
            for i in range(2):
                acc[i] = acc[i] + xrecv[s, d, i].astype(F32)
        g, u = acc
        hbuf[s, core, x] = (g / (1.0 + jnp.exp(-g)) * u).astype(BF16)
        for d in range(1, xs):
            h_copy(s, d).start()

    def hc_copy(s):
        return remote(hbuf.at[s, core], hbuf.at[s, core], ch_s.at[s], ch_r.at[s], peer_core)

    def share(s):
        for d in range(1, xs):
            h_copy(s, d).wait_recv()
        hc_copy(s).start()

    def settle(s):
        hc_copy(s).wait_recv()

    def run(stages, group):
        for stage in stages:
            for j, h in group:
                stage(j * 2 + h)

    def rest(group):
        run((fold_core, activate, share, settle), group)

    middle = has_left & has_right
    outer = jnp.logical_not(middle)
    last = line - 1
    second = [(j, 1) for j in range(last - 1, -1, -1)]
    third = [(last, 0), (last, 1)]

    project(0, 0)
    rest([(0, 0)])

    @pl.when(middle)
    def _():
        for low in range(1, last, 2):
            for q in range(HALVES):
                for j in range(low, min(low + 2, last)):
                    take(j, q)

    for j in range(1, last):

        @pl.when(outer)
        def _():
            for q in range(HALVES):
                take(j, q)

        project(j, 0)
    rest([(j, 0) for j in range(1, last)])

    @pl.when(middle)
    def _():
        for q in range(HALVES):
            take(last, q)

    far = reduce_orders(line)
    targets = [pick([far[i][n] for i in range(line)], a) for n in range(last)]
    spots = [pick([arrive[i].index(far[i][n]) for i in range(line)], a) for n in range(last)]

    def term(j, q):
        acc = None
        for h in range(2):
            hid = hbuf[j * 2 + h].reshape(tokens, units)
            t = jnp.dot(hid, wd[h, q], preferred_element_type=F32)
            acc = t if acc is None else acc + t
        return acc

    def p_right(b, q):
        return remote(psend.at[b, q], pleft.at[b, q], p_s.at[b, q], pl_r.at[b, q], right)

    def p_left(b, q):
        return remote(psend.at[b, q], pright.at[b, q], p_s.at[b, q], pr_r.at[b, q], left)

    def reduce(n):
        b = targets[n]
        for q in range(PIECES):
            if n == 0:
                d_copy(q).wait_recv()
            pown[...] = term(spots[n], q)

            @pl.when((b > a) & has_left)
            def _():
                p_right(b, q).wait_recv()
                pown[...] += pleft[b, q].astype(F32)

            @pl.when((b < a) & has_right)
            def _():
                p_left(b, q).wait_recv()
                pown[...] += pright[b, q].astype(F32)

            psend[b, q] = pown[...].astype(BF16)

            @pl.when(b > a)
            def _():
                p_right(b, q).start()

            @pl.when(b < a)
            def _():
                p_left(b, q).start()

    w_copy.wait_recv()
    for j, h in second:
        project(j, h)

    @pl.when(middle)
    def _():
        for j, h in third:
            project(j, h)
        rest(second + third)
        reduce(0)

    @pl.when(outer)
    def _():
        run((fold_core, activate), second)
        for q in range(HALVES):
            take(last, q)
        for j, h in third:
            project(j, h)
        run((fold_core,), third)
        run((share, settle), second)
        reduce(0)
        run((activate, share, settle), third)

    for n in range(1, last):
        reduce(n)

    for q in range(PIECES):
        pown[...] = term(0, q)

        @pl.when(has_left)
        def _():
            p_right(a, q).wait_recv()
            pown[...] += pleft[a, q].astype(F32)

        @pl.when(has_right)
        def _():
            p_left(a, q).wait_recv()
            pown[...] += pright[a, q].astype(F32)

        obuf[:, pl.ds(q * size, size)] = pown[...].astype(BF16)
        pltpu.make_async_copy(
            obuf.at[:, pl.ds(q * size, size)], out_hbm.at[:, pl.ds(q * size, size)], loc.at[4 + q]
        ).start()

    w_copy.wait_send()
    for q in range(PIECES):
        d_copy(q).wait_send()
    for j in range(line):
        b = order[j]

        for q in range(HALVES):

            @pl.when((b <= a) & has_right)
            def _():
                go_right(b, q).wait_send()

            @pl.when((b >= a) & has_left)
            def _():
                go_left(b, q).wait_send()

        if j:
            for q in range(PIECES):
                p_right(b, q).wait_send()
        for h in range(2):
            s = j * 2 + h
            core_copy(s).wait_send()
            hc_copy(s).wait_send()
            for d in range(1, xs):
                x_copy(s, d).wait_send()
                h_copy(s, d).wait_send()
    for q in range(PIECES):
        pltpu.make_async_copy(
            obuf.at[:, pl.ds(q * size, size)], out_hbm.at[:, pl.ds(q * size, size)], loc.at[4 + q]
        ).wait()


def per_device(n_row, n_col, tokens, gate, up, down, gmask, umask, dmask):
    line, xs = n_col // PAIR, n_row // 2
    t, k = tokens.shape
    units = gate.shape[1]
    wide = down.shape[1]
    half = t // 2
    part = half // xs
    steps = 2 * line
    dma = pltpu.SemaphoreType.DMA
    vmem = pltpu.VMEM
    hbm = pl.BlockSpec(memory_space=pl.ANY)
    smem = pl.BlockSpec(memory_space=pltpu.SMEM)
    size = wide // PIECES
    return pl.pallas_call(
        functools.partial(kernel, line, xs, gmask.shape, dmask.shape),
        out_shape=jax.ShapeDtypeStruct((t, wide), BF16),
        in_specs=[hbm] * 4 + [smem] * 3,
        out_specs=hbm,
        scratch_shapes=[
            vmem((line, HALVES, half, k), BF16),
            vmem((2, k, units), BF16),
            vmem((units, wide), BF16),
            vmem((2, 2, k, units), BF16),
            vmem((2, PIECES, units, size), BF16),
            vmem((steps, 2, half, units), BF16),
            vmem((steps, 2, half, units), BF16),
            vmem((steps, HALVES, 2, half, units), F32),
            vmem((steps, xs, 2, part, units), BF16),
            vmem((steps, xs, 2, part, units), BF16),
            vmem((steps, 2, xs, part, units), BF16),
            vmem((line, PIECES, t, size), BF16),
            vmem((line, PIECES, t, size), BF16),
            vmem((line, PIECES, t, size), BF16),
            vmem((t, size), F32),
            vmem((t, wide), BF16),
            dma((4 + PIECES,)),
            dma((line, HALVES)), dma((line, HALVES)), dma((line, HALVES)),
            dma((2,)), dma((PIECES,)), dma((PIECES,)),
            dma((steps,)), dma((steps,)),
            dma((steps, xs)), dma((steps, xs)),
            dma((steps, xs)), dma((steps, xs)),
            dma((steps,)), dma((steps,)),
            dma((line, PIECES)), dma((line, PIECES)), dma((line, PIECES)),
        ],
        compiler_params=pltpu.CompilerParams(
            collective_id=0, has_side_effects=True, vmem_limit_bytes=60 * 1024 * 1024
        ),
    )(tokens.reshape(HALVES, half, k), gate, up, down, *(m.reshape(-1) for m in (gmask, umask, dmask)))


def solution(mesh):
    n_row, n_col = mesh.shape["row"], mesh.shape["col"]
    return jax.shard_map(
        functools.partial(per_device, n_row, n_col),
        mesh=mesh,
        in_specs=(
            P("col", "row"),
            P("row", "col"),
            P("row", "col"),
            P("col", "row"),
            P("row", "col"),
            P("row", "col"),
            P("col", "row"),
        ),
        out_specs=P("col", "row"),
        check_vma=False,
    )
```
